32 devices in a mesh: blk: 16 (over z, x, core), head: 2 (over y).
Axes of the slice: x: 2, y: 2, z: 4, core: 2. Of those that a mesh axis runs over, the one named last changes fastest.
Arguments:
- query: bfloat16 [2, 8192, 128], P('head', 'blk'), may hold values from -12 to 12
- key: bfloat16 [8192, 128], P('blk'), may hold values from -6 to 6
- value: bfloat16 [8192, 128], P('blk'), may hold values from -6 to 6
- output: bfloat16 [2, 8192, 128], P('head', 'blk'), may hold values from -6 to 6
- out_grad: bfloat16 [2, 8192, 128], P('head', 'blk'), may hold values from -6 to 6
- lse: float32 [2, 8192], P('head', 'blk'), may hold values from 5 to 14
- block_order: int32 [32], replicated, may hold values from 0 to 31, as said below
Outputs:
- grad_query: float32 [2, 8192, 128], P('head', 'blk')
- grad_key: float32 [8192, 128], P(('blk', 'head'))
- grad_value: float32 [8192, 128], P(('blk', 'head'))
The draws below stay inside these ranges and needn't reach their ends.
Inputs may be any that keep to these rules, and one draw needn't show every extreme that they name: A permutation of 0 to 31; the storage block j, rows j * 256 to (j + 1) * 256 - 1, holds the sequence block block_order[j].
All inputs are finite; a program needn't handle non-finite values.
Results may differ from the reference program's by a relative error of at most 0.0036.
Values may be sent and summed in bfloat16 or wider, within the bound.
No kernel may reach another device: no remote copies, remote signals or barrier semaphores. Data moves between devices by JAX's collectives and lax.ppermute only.
A program may use at most 64 MiB of HBM per device.

```python
import jax
import jax.numpy as jnp
from jax import lax

DH = 128
BLOCK = 256
NBLOCKS = 32
SEQ = 8192
HEADS = 2


def block_table(key):
    return jax.random.permutation(jax.random.fold_in(key, 11), NBLOCKS).astype(jnp.int32)


def draw_block_order(key, part):
    return block_table(key)


def draw_lse(key, part):
    table = block_table(key)
    rows = jnp.arange(SEQ, dtype=jnp.int32)
    pos = table[rows // BLOCK] * BLOCK + rows % BLOCK
    base = jnp.log(pos.astype(jnp.float32) + 64.0) + 2.0
    noise_key = jax.random.fold_in(key, 23)
    noise = jax.random.uniform(noise_key, (HEADS, SEQ), jnp.float32, -0.5, 0.5)
    return base[None, :] + noise


def steps_of(own_key, shape, cuts, low, high):
    loudness, own = 1.0, jax.random.fold_in(own_key, 6)
    for position, blocks in cuts:
        steps = jnp.exp(jax.random.uniform(jax.random.fold_in(own, position), (blocks,), jnp.float32, low / len(cuts), high / len(cuts)))
        loudness = loudness * jnp.repeat(steps, shape[position] // blocks).reshape([-1 if axis == position else 1 for axis in range(len(shape))])
    return loudness


def bell_draw(rng, dims, deviation, most, shards=(), kind=jnp.bfloat16):
    drawn = deviation * jax.random.normal(rng, dims, jnp.float32)
    if shards:
        drawn = drawn * steps_of(rng, dims, shards, -0.22, 0.18)
    return jnp.clip(drawn, -most, most).astype(kind)


def setup_inputs(seed: int = 0) -> dict:
    key_of = jax.random.split(jax.random.key(seed), 8)
    query = bell_draw(key_of[0], (HEADS, SEQ, DH), 2.0, 12.0, ((0, 2), (1, 16)))
    key = bell_draw(key_of[1], (SEQ, DH), 1.0, 6.0, ((0, 16),))
    value = bell_draw(key_of[2], (SEQ, DH), 1.0, 6.0, ((0, 16),))
    output = bell_draw(key_of[3], (HEADS, SEQ, DH), 1.0, 6.0, ((0, 2), (1, 16)))
    out_grad = bell_draw(key_of[4], (HEADS, SEQ, DH), 1.0, 6.0, ((0, 2), (1, 16)))
    lse = draw_lse(jax.random.fold_in(key_of[7], 71), 0)
    block_order = draw_block_order(jax.random.fold_in(key_of[7], 71), 0)
    return dict(query=query, key=key, value=value, output=output, out_grad=out_grad, lse=lse, block_order=block_order)


def positions(block_order):
    rows = jnp.arange(SEQ, dtype=jnp.int32)
    return block_order[rows // BLOCK].astype(jnp.int32) * BLOCK + rows % BLOCK


def reference(query, key, value, output, out_grad, lse, block_order):
    scale = DH ** -0.5
    pos = positions(block_order)
    delta = jnp.sum(out_grad.astype(jnp.float32) * output.astype(jnp.float32), axis=-1)
    key_wide = key.astype(jnp.float32)
    value_wide = value.astype(jnp.float32)
    count = SEQ // BLOCK

    def step(carry, index):
        grad_k, grad_v = carry
        start = index * BLOCK
        q_rows = lax.dynamic_slice_in_dim(query, start, BLOCK, 1).astype(jnp.float32)
        g_rows = lax.dynamic_slice_in_dim(out_grad, start, BLOCK, 1).astype(jnp.float32)
        l_rows = lax.dynamic_slice_in_dim(lse, start, BLOCK, 1)
        d_rows = lax.dynamic_slice_in_dim(delta, start, BLOCK, 1)
        q_pos = lax.dynamic_slice_in_dim(pos, start, BLOCK, 0)
        scores = jnp.einsum("hqd,kd->hqk", q_rows, key_wide) * scale
        live = q_pos[:, None] >= pos[None, :]
        probs = jnp.where(live[None], jnp.exp(scores - l_rows[..., None]), 0.0)
        probs_low = probs.astype(jnp.bfloat16).astype(jnp.float32)
        dprobs = jnp.einsum("hqd,kd->hqk", g_rows, value_wide)
        dscores = (probs * (dprobs - d_rows[..., None])).astype(jnp.bfloat16).astype(jnp.float32)
        grad_q = jnp.einsum("hqk,kd->hqd", dscores, key_wide) * scale
        grad_k = grad_k + jnp.einsum("hqk,hqd->kd", dscores, q_rows) * scale
        grad_v = grad_v + jnp.einsum("hqk,hqd->kd", probs_low, g_rows)
        return (grad_k, grad_v), grad_q

    empty = jnp.zeros((SEQ, DH), jnp.float32)
    (grad_key, grad_value), blocks = lax.scan(step, (empty, empty), jnp.arange(count, dtype=jnp.int32))
    grad_query = jnp.transpose(blocks, (1, 0, 2, 3)).reshape(HEADS, SEQ, DH)
    return grad_query, grad_key, grad_value
```

```python
import functools

import jax
import jax.numpy as jnp
from jax import lax
from jax.experimental import pallas as pl
from jax.experimental.pallas import tpu as pltpu
from jax.sharding import PartitionSpec as P

LOG2E = 1.4426950408889634
WIDTH = 4


def contract(left, right, dims):
    return lax.dot_general(left, right, (dims, ((), ())), preferred_element_type=jnp.float32)


def tile_kernel(shape, *refs):
    q_units, k_units, split, block, width, scale = shape
    n_q, n_k = 2 * len(q_units), 2 * len(k_units)
    refs = list(refs)

    def take(count):
        taken, refs[:] = refs[:count], refs[count:]
        return taken

    (order,) = take(1)
    q_in, g_in, s_in = take(len(q_units)), take(len(q_units)), take(len(q_units))
    k_in, v_in = take(n_k), take(n_k)
    dq_out, dkv_out = take(len(q_units)), take(n_k)
    q, g, s, k, v, dq, dk, dv, q_at, k_at, live, count = refs

    me = lax.axis_index("blk")
    head = lax.axis_index("head")
    for u, offset in enumerate(q_units):
        for half in range(2):
            q[2 * u + half] = q_in[u][half * block : (half + 1) * block]
            g[2 * u + half] = g_in[u][half * block : (half + 1) * block]
            s[2 * u + half] = s_in[u][:, half * block : (half + 1) * block]
            q_at[2 * u + half] = order[2 * (me ^ offset) + half]
    for u, offset in enumerate(k_units):
        for part in range(2):
            half = (part + head) % 2 if split else part
            k[2 * u + part] = k_in[2 * u + part][...]
            v[2 * u + part] = v_in[2 * u + part][...]
            k_at[2 * u + part] = order[2 * (me ^ offset) + half]
    dk[...] = jnp.zeros_like(dk)
    dv[...] = jnp.zeros_like(dv)

    row = n_k + WIDTH
    for i in range(n_q):
        found = jnp.int32(0)
        for j in range(n_k):
            live[i * row + found] = jnp.int32(j)
            found += (q_at[i] >= k_at[j]).astype(jnp.int32)
        for e in range(WIDTH - 1):
            live[i * row + found + e] = jnp.int32(-1)
        count[i] = found

    ahead = lax.broadcasted_iota(jnp.int32, (block, block), 1) - lax.broadcasted_iota(
        jnp.int32, (block, block), 0
    )

    def each_q(i, _):
        q_rows, g_rows = q[i], g[i]
        low = s[i, 0:1, :] * LOG2E
        delta = s[i, 1:2, :]
        dq[i] = jnp.zeros((block, width), jnp.float32)

        def each_group(t, _):
            named = [live[i * row + t * WIDTH + e] for e in range(WIDTH)]
            at = [jnp.maximum(j, 0) for j in named]
            least = [
                jnp.where(j < 0, 2 * block, (k_at[a] - q_at[i]) * block) for j, a in zip(named, at)
            ]
            scores = [contract(k[a], q_rows, ((1,), (1,))) for a in at]
            dprobs = [contract(v[a], g_rows, ((1,), (1,))) for a in at]
            probs = [
                jnp.where(ahead >= m, jnp.exp2(x * (scale * LOG2E) - low), 0.0)
                for x, m in zip(scores, least)
            ]
            dscores = [(p * (x - delta)).astype(jnp.bfloat16) for p, x in zip(probs, dprobs)]
            probs_low = [p.astype(jnp.bfloat16) for p in probs]
            total = sum(contract(d, k[a], ((0,), (0,))) for d, a in zip(dscores, at))
            dq[i] += total
            for a, p, d in zip(at, probs_low, dscores):
                dv[a] += contract(p, g_rows, ((1,), (0,)))
                dk[a] += contract(d, q_rows, ((1,), (0,)))
            return 0

        lax.fori_loop(0, (count[i] + WIDTH - 1) // WIDTH, each_group, 0)
        return 0

    lax.fori_loop(0, n_q, each_q, 0)
    for u in range(len(q_units)):
        for half in range(2):
            dq_out[u][half * block : (half + 1) * block] = (dq[2 * u + half] * scale).astype(
                dq_out[u].dtype
            )
    for j in range(n_k):
        dkv_out[j][0] = (dk[j] * scale).astype(dkv_out[j].dtype)
        dkv_out[j][1] = dv[j].astype(dkv_out[j].dtype)


def tile_grads(order, q, g, s, k, v, q_units, k_units, split, scale):
    rows, width = q[0].shape
    block = rows // 2
    n_q, n_k = 2 * len(q_units), 2 * len(k_units)
    vmem = pl.BlockSpec(memory_space=pltpu.VMEM)
    smem = pl.BlockSpec(memory_space=pltpu.SMEM)
    out_shape = [
        jax.ShapeDtypeStruct((rows, width), jnp.bfloat16 if offset else jnp.float32)
        for offset in q_units
    ] + [
        jax.ShapeDtypeStruct((2, block, width), jnp.bfloat16 if offset & 1 else jnp.float32)
        for offset in k_units
        for _ in range(2)
    ]
    pairs = n_q * n_k // 2
    outs = pl.pallas_call(
        functools.partial(tile_kernel, (q_units, k_units, split, block, width, scale)),
        out_shape=out_shape,
        in_specs=[smem] + [vmem] * (3 * len(q_units) + 2 * n_k),
        out_specs=[vmem] * len(out_shape),
        scratch_shapes=[
            pltpu.VMEM((n_q, block, width), jnp.bfloat16),
            pltpu.VMEM((n_q, block, width), jnp.bfloat16),
            pltpu.VMEM((n_q, 2, block), jnp.float32),
            pltpu.VMEM((n_k, block, width), jnp.bfloat16),
            pltpu.VMEM((n_k, block, width), jnp.bfloat16),
            pltpu.VMEM((n_q, block, width), jnp.float32),
            pltpu.VMEM((n_k, block, width), jnp.float32),
            pltpu.VMEM((n_k, block, width), jnp.float32),
            pltpu.SMEM((n_q,), jnp.int32),
            pltpu.SMEM((n_k,), jnp.int32),
            pltpu.SMEM((n_q * (n_k + WIDTH),), jnp.int32),
            pltpu.SMEM((n_q,), jnp.int32),
        ],
        cost_estimate=pl.CostEstimate(
            flops=pairs * block * block * width * 10,
            bytes_accessed=(n_q + n_k) * block * width * 8,
            transcendentals=pairs * block * block,
        ),
        name="tile_grads",
    )(order, *q, *g, *s, *k, *v)
    return outs[: len(q_units)], outs[len(q_units) :]


def offsets_of(bits):
    found = [0]
    for bit in bits:
        found = found + [o | 1 << bit for o in found]
    return tuple(sorted(found))


def on_device(query, key, value, output, out_grad, lse, block_order):
    scale = key.shape[1] ** (-0.5)
    rows = key.shape[0]
    block = rows // 2
    devices = lax.axis_size("blk")
    heads = lax.axis_size("head")
    bits = devices.bit_length() - 1
    q_bits = tuple(range(bits))[1:3]
    k_bits = tuple(b for b in range(bits) if b not in q_bits)
    q_units, k_units = offsets_of(q_bits), offsets_of(k_bits)
    split = heads == 2

    def across(array, offset):
        return lax.ppermute(array, "blk", [(i, i ^ offset) for i in range(devices)])

    def other_head(array):
        return lax.ppermute(array, "head", [(0, 1), (1, 0)])

    delta = jnp.sum(out_grad[0].astype(jnp.float32) * output[0].astype(jnp.float32), axis=1)
    stats = jnp.concatenate([lse, delta[None]])

    def gather(mine, order):
        held = {0: mine}
        for bit in order:
            held |= {o | 1 << bit: across(held[o], 1 << bit) for o in list(held)}
        return [held[o] for o in q_units]

    q = gather(query[0], q_bits)
    g = gather(out_grad[0], q_bits[::-1])
    s = gather(stats, q_bits)

    def gather_blocks(whole):
        if split:
            head = lax.axis_index("head")
            held = {
                (0, 0): lax.dynamic_slice_in_dim(whole, head * block, block, 0),
                (0, 1): lax.dynamic_slice_in_dim(whole, (1 - head) * block, block, 0),
            }
        else:
            held = {(0, 0): whole[:block], (0, 1): whole[block:]}
        for bit in k_bits[::-1]:
            for o in [o for o, part in held if part == 0]:
                far = o | 1 << bit
                held[far, 0] = across(held[o, 0], 1 << bit)
                if split and bit:
                    held[far, 1] = other_head(held[far, 0])
                else:
                    held[far, 1] = across(held[o, 1], 1 << bit)
        return [held[o, part] for o in k_units for part in range(2)]

    k, v = gather_blocks(key), gather_blocks(value)
    dq, dkv = tile_grads(block_order, q, g, s, k, v, q_units, k_units, split, scale)

    held = {(o, part): dkv[2 * u + part] for u, o in enumerate(k_units) for part in range(2)}

    def fold(bit, parts):
        for o, part in [at for at in held if at[0] >> bit & 1 and at[1] in parts]:
            near = o ^ 1 << bit
            sent = across(held.pop((o, part)).astype(jnp.bfloat16), 1 << bit)
            held[near, part] = held[near, part] + sent.astype(jnp.float32)

    if split:
        fold(0, (1,))
        fold(0, (0,))
        for o in sorted({o for o, _ in held}, reverse=True):
            sent = other_head(held.pop((o, 1)).astype(jnp.bfloat16))
            held[o, 0] = held[o, 0] + sent.astype(jnp.float32)
        for bit in k_bits[:0:-1]:
            fold(bit, (0,))
        own_k, own_v = held[0, 0][0], held[0, 0][1]
    else:
        for bit in (0,) + k_bits[:0:-1]:
            fold(bit, (0, 1))
        own_k, own_v = (
            lax.psum_scatter(
                jnp.concatenate([held[0, 0][t], held[0, 1][t]]),
                "head",
                scatter_dimension=0,
                tiled=True,
            )
            for t in range(2)
        )
    grad_q = dq[0]
    for part, offset in zip(dq[1:], q_units[1:]):
        grad_q = grad_q + across(part, offset).astype(jnp.float32)
    return (grad_q[None], own_k, own_v)


def solution(mesh):
    in_specs = (
        P("head", "blk", None),
        P("blk", None),
        P("blk", None),
        P("head", "blk", None),
        P("head", "blk", None),
        P("head", "blk"),
        P(),
    )
    out_specs = (P("head", "blk", None), P(("blk", "head"), None), P(("blk", "head"), None))
    return jax.shard_map(
        on_device, mesh=mesh, in_specs=in_specs, out_specs=out_specs, check_vma=False
    )
```

```python
import functools

import jax
import jax.numpy as jnp
from jax import lax
from jax.experimental import pallas as pl
from jax.experimental.pallas import tpu as pltpu
from jax.sharding import PartitionSpec as P


LOG2E = 1.4426950408889634
WIDTH = 4
LIMIT = 24 * 2**20
VMEM = pl.BlockSpec(memory_space=pltpu.VMEM)
SMEM = pl.BlockSpec(memory_space=pltpu.SMEM)


def contract(left, right, dims):
    return lax.dot_general(left, right, (dims, ((), ())), preferred_element_type=jnp.float32)


def pieces_of(row):
    found = []
    for _ in range(3):
        piece = row.astype(jnp.bfloat16).astype(jnp.float32)
        found.append(piece)
        row = row - piece
    return found


def pack_kernel(split, *refs):
    given, (sent, kv_mine, kv_all), local, done = refs[:6], refs[6:9], refs[9:15], refs[15]
    copies = [pltpu.make_async_copy(a, b, done.at[n]) for n, (a, b) in enumerate(zip(given, local))]
    for copy in copies:
        copy.start()
    for copy in copies:
        copy.wait()
    k, v, q, g, o, low = local
    rows, width = q.shape
    block = rows // 2
    head = lax.axis_index("head")
    for part in range(2):
        half = lax.rem(head + part, 2) if split else part
        at = pl.ds(pl.multiple_of(half * block, block), block)
        kv_all[2 * part] = k[at, :]
        kv_all[2 * part + 1] = v[at, :]
        if part == 0:
            kv_mine[0] = k[at, :]
            kv_mine[1] = v[at, :]
    sent[:rows] = q[...]
    sent[rows : 2 * rows] = g[...]
    product = g[...].astype(jnp.float32) * o[...].astype(jnp.float32)
    delta = jnp.sum(product.T, axis=0, keepdims=True)
    lines = [
        piece[:, at : at + width]
        for row in (low[...] * LOG2E, delta)
        for piece in pieces_of(row)
        for at in range(0, rows, width)
    ]
    pad = sent.shape[0] - 2 * rows - len(lines)
    lines.append(jnp.zeros((pad, width), jnp.float32))
    sent[2 * rows :] = jnp.concatenate(lines, axis=0).astype(jnp.bfloat16)


def pack(query, output, out_grad, lse, key, value, split):
    rows, width = query.shape
    block = rows // 2
    lines = -(-6 * (rows // width) // 16) * 16
    given = (key, value, query, out_grad, output, lse)
    return pl.pallas_call(
        functools.partial(pack_kernel, split),
        out_shape=[
            jax.ShapeDtypeStruct((2 * rows + lines, width), jnp.bfloat16),
            jax.ShapeDtypeStruct((2, block, width), jnp.bfloat16),
            jax.ShapeDtypeStruct((4, block, width), jnp.bfloat16),
        ],
        in_specs=[pl.BlockSpec(memory_space=pltpu.HBM)] * len(given),
        out_specs=[VMEM] * 3,
        scratch_shapes=[pltpu.VMEM(a.shape, a.dtype) for a in given]
        + [pltpu.SemaphoreType.DMA((len(given),))],
        compiler_params=pltpu.CompilerParams(vmem_limit_bytes=LIMIT),
        name="pack",
    )(*[pltpu.with_memory_space_constraint(a, pltpu.HBM) for a in given])


def tile_kernel(shape, *refs):
    q_units, q_held, q_done, k_units, n_kv, k_held, k_done, split, rows, width, scale = shape
    block = rows // 2
    n_q, n_k = 2 * len(q_units), 2 * len(k_units)
    refs = list(refs)

    def take(count):
        taken, refs[:] = refs[:count], refs[count:]
        return taken

    (order,) = take(1)
    q_in, kv_in = take(len(q_units)), take(n_kv)
    q_before = dict(zip(q_held, take(len(q_held))))
    k_before = take(1)[0] if k_held else None
    dq_out = dict(zip(q_units, take(len(q_units))))
    sent, kept = take(2) if k_done else (None, take(1)[0])
    q, g, low, delta, k, v, kt, dqt, total, q_at, k_at, pair_q, pair_k = refs

    me = lax.axis_index("blk")
    head = lax.axis_index("head")
    lines = rows // width
    for u, offset in enumerate(q_units):
        stats = q_in[u][2 * rows :].astype(jnp.float32)
        for half in range(2):
            i = 2 * u + half
            q[i] = q_in[u][half * block : (half + 1) * block]
            g[i] = q_in[u][rows + half * block : rows + (half + 1) * block]
            for kind, out in enumerate((low, delta)):
                pieces = [
                    stats[(3 * kind + p) * lines : (3 * kind + p + 1) * lines] for p in range(3)
                ]
                row = pieces[0] + pieces[1] + pieces[2]
                start = half * (lines // 2)
                out[i] = jnp.concatenate(
                    [row[c : c + 1] for c in range(start, start + lines // 2)], axis=1
                )
            q_at[i] = order[2 * (me ^ offset) + half]
            if offset in q_before:
                dqt[i] = q_before[offset][half]
            else:
                dqt[i] = jnp.zeros((width, block), jnp.float32)
    blocks = [(ref, at) for ref in kv_in for at in range(0, ref.shape[0], 2)]
    for j, (ref, at) in enumerate(blocks):
        k[j] = ref[at]
        v[j] = ref[at + 1]
        kt[j] = ref[at].T
        half = lax.rem(head + j % 2, 2) if split else j % 2
        k_at[j] = order[2 * (me ^ k_units[j // 2]) + half]
    total[...] = k_before[...] if k_held else jnp.zeros_like(total)

    found = jnp.int32(0)
    for i in range(n_q):
        at = q_at[i]
        for j in range(n_k):
            pair_q[found] = jnp.int32(i)
            pair_k[found] = jnp.int32(j)
            found += (at >= k_at[j]).astype(jnp.int32)
    for e in range(WIDTH - 1):
        pair_q[found + e] = jnp.int32(0)
        pair_k[found + e] = jnp.int32(-1)

    ahead = lax.broadcasted_iota(jnp.int32, (block, block), 1) - lax.broadcasted_iota(
        jnp.int32, (block, block), 0
    )

    def each_group(t, _):
        at_q = [pair_q[t * WIDTH + e] for e in range(WIDTH)]
        named = [pair_k[t * WIDTH + e] for e in range(WIDTH)]
        at_k = [jnp.maximum(j, 0) for j in named]
        probs_low, dscores = [], []
        for i, j, name in zip(at_q, at_k, named):
            least = jnp.where(name < 0, 2 * block, (k_at[j] - q_at[i]) * block)
            scores = contract(k[j], q[i], ((1,), (1,)))
            dprobs = contract(v[j], g[i], ((1,), (1,)))
            probs = jnp.where(ahead >= least, jnp.exp2(scores * (scale * LOG2E) - low[i]), 0.0)
            probs_low.append(probs.astype(jnp.bfloat16))
            dscores.append((probs * (dprobs - delta[i])).astype(jnp.bfloat16))
        part_v = [contract(p, g[i], ((1,), (0,))) for p, i in zip(probs_low, at_q)]
        part_k = [contract(d, q[i], ((1,), (0,))) for d, i in zip(dscores, at_q)]
        part_q = [contract(kt[j], d, ((1,), (0,))) for d, j in zip(dscores, at_k)]
        for i, j, a, b, c in zip(at_q, at_k, part_k, part_v, part_q):
            total[2 * j] += a
            total[2 * j + 1] += b
            dqt[i] += c
        return 0

    lax.fori_loop(0, (found + WIDTH - 1) // WIDTH, each_group, 0)
    for u, offset in enumerate(q_units):
        out = dq_out[offset]
        for half in range(2):
            if offset in q_done:
                got = (dqt[2 * u + half] * scale).T.astype(out.dtype)
                out[half * block : (half + 1) * block] = got
            else:
                out[half] = dqt[2 * u + half]
    if k_done:
        place = {0: 0, 1: 0}
        for u, offset in enumerate(k_units):
            out = sent if offset & 1 else kept
            for j in (2 * u, 2 * u + 1):
                at = place[offset & 1]
                out[at] = (total[2 * j] * scale).astype(out.dtype)
                out[at + 1] = total[2 * j + 1].astype(out.dtype)
                place[offset & 1] = at + 2
    else:
        kept[...] = total[...]


def tile_grads(order, q, kv, q_before, k_before, q_done, k_done, split, rows, scale):
    q_units, k_units = tuple(q), tuple(kv)
    kv = [a for o in k_units for a in kv[o]]
    width = kv[0].shape[2]
    block = rows // 2
    n_q, n_k = 2 * len(q_units), 2 * len(k_units)
    out_shape = []
    for offset in q_units:
        if offset not in q_done:
            out_shape.append(jax.ShapeDtypeStruct((2, width, block), jnp.float32))
        else:
            kind = jnp.bfloat16 if offset else jnp.float32
            out_shape.append(jax.ShapeDtypeStruct((rows, width), kind))
    if k_done:
        out_shape.append(jax.ShapeDtypeStruct((n_k, block, width), jnp.bfloat16))
        out_shape.append(jax.ShapeDtypeStruct((n_k, block, width), jnp.float32))
    else:
        out_shape.append(jax.ShapeDtypeStruct((2 * n_k, block, width), jnp.float32))
    pairs = n_q * n_k // 2
    q_held = tuple(o for o in q_units if o in q_before)
    k_held = k_before is not None
    operands = [*q.values(), *kv, *(q_before[o] for o in q_held)] + ([k_before] if k_held else [])
    shape = (q_units, q_held, q_done, k_units, len(kv), k_held, k_done, split, rows, width, scale)
    outs = pl.pallas_call(
        functools.partial(tile_kernel, shape),
        out_shape=out_shape,
        in_specs=[SMEM] + [VMEM] * len(operands),
        out_specs=[VMEM] * len(out_shape),
        scratch_shapes=[
            pltpu.VMEM((n_q, block, width), jnp.bfloat16),
            pltpu.VMEM((n_q, block, width), jnp.bfloat16),
            pltpu.VMEM((n_q, 1, block), jnp.float32),
            pltpu.VMEM((n_q, 1, block), jnp.float32),
            pltpu.VMEM((n_k, block, width), jnp.bfloat16),
            pltpu.VMEM((n_k, block, width), jnp.bfloat16),
            pltpu.VMEM((n_k, width, block), jnp.bfloat16),
            pltpu.VMEM((n_q, width, block), jnp.float32),
            pltpu.VMEM((2 * n_k, block, width), jnp.float32),
            pltpu.SMEM((n_q,), jnp.int32),
            pltpu.SMEM((n_k,), jnp.int32),
            pltpu.SMEM((n_q * n_k + WIDTH,), jnp.int32),
            pltpu.SMEM((n_q * n_k + WIDTH,), jnp.int32),
        ],
        cost_estimate=pl.CostEstimate(
            flops=pairs * block * block * width * 10,
            bytes_accessed=(n_q + n_k) * block * width * 8,
            transcendentals=pairs * block * block,
        ),
        compiler_params=pltpu.CompilerParams(vmem_limit_bytes=LIMIT),
        name="tile_grads",
    )(order, *operands)
    return dict(zip(q_units, outs)), outs[len(q_units) :]


def offsets_of(bits):
    found = [0]
    for bit in bits:
        found = found + [o | 1 << bit for o in found]
    return tuple(sorted(found))


def share_kernel(places, kept, got, *outs):
    for out, (at, size) in zip(outs, places):
        if size == 1:
            out[...] = (kept[at] + got[at].astype(jnp.float32)).astype(out.dtype)
        else:
            for n in range(size):
                out[n] = (kept[at + n] + got[at + n].astype(jnp.float32)).astype(out.dtype)


def share(kept, got, kinds):
    size = kept.shape[0] // len(kinds)
    places, shapes = [], []
    for n, group in enumerate(kinds):
        each = size // len(group)
        for e, kind in enumerate(group):
            places.append((n * size + e * each, each))
            lead = kept.shape[1:] if each == 1 else (each,) + kept.shape[1:]
            shapes.append(jax.ShapeDtypeStruct(lead, kind))
    return pl.pallas_call(
        functools.partial(share_kernel, tuple(places)),
        out_shape=shapes,
        in_specs=[VMEM] * 2,
        out_specs=[VMEM] * len(shapes),
        compiler_params=pltpu.CompilerParams(vmem_limit_bytes=LIMIT),
        name="share",
    )(kept, got)


def on_device(query, key, value, output, out_grad, lse, block_order):
    rows, width = key.shape
    scale = width ** (-0.5)
    devices = lax.axis_size("blk")
    heads = lax.axis_size("head")
    bits = devices.bit_length() - 1
    q_bits = tuple(range(bits))[1:3]
    k_bits = tuple(b for b in range(bits) if b not in q_bits)
    q_units, k_units = offsets_of(q_bits), offsets_of(k_bits)
    split = heads == 2

    def across(array, offset):
        return lax.ppermute(array, "blk", [(i, i ^ offset) for i in range(devices)])

    def across_both(array, offset):
        route = [(2 * i + h, 2 * (i ^ offset) + 1 - h) for i in range(devices) for h in range(2)]
        return lax.ppermute(array, ("blk", "head"), route)

    sent, kv_mine, kv_all = pack(query[0], output[0], out_grad[0], lse, key, value, split)

    held = {0: [kv_all]}
    for bit in k_bits[:0:-1]:
        for o in list(held):
            if split and o == 0:
                mine = across(kv_mine, 1 << bit)
                held[1 << bit] = [mine, across_both(mine, 0)]
            else:
                far = [across(a, 1 << bit) for a in held[o]]
                held[o | 1 << bit] = far
    q = {o: across(sent, o) if o else sent for o in q_units}
    for o in list(held):
        held[o | 1] = [across(a, 1) for a in held[o]]

    def some(array_of, units):
        return {o: array_of[o] for o in units}

    home = [o for o in k_units if o < 2]
    away = [o for o in k_units if o >= 2]
    early, late = q_units[:-1], q_units[-1:]
    tile = functools.partial(tile_grads, block_order, split=split, rows=rows, scale=scale)
    held_q, (total,) = tile(some(q, early), some(held, home), {}, None, (), False)
    dq, (far_sent, far_kept) = tile(some(q, q_units), some(held, away), held_q, None, early, True)
    held_q = some(dq, late)
    far_got = across(far_sent, 1)
    last_q, (home_sent, home_kept) = tile(
        some(q, late), some(held, home), held_q, total, late, True
    )
    dq |= last_q
    home_got = across(home_sent, 1)

    low, wide = jnp.bfloat16, jnp.float32
    far_offsets = [o for o in away if not o & 1]
    arrived = []
    if split:
        far = share(far_kept, far_got, [(wide, low), (low, low)] * len(far_offsets))
        for n, offset in enumerate(far_offsets):
            (mine_k, mine_v), (other_k, other_v) = far[4 * n : 4 * n + 2], far[4 * n + 2 : 4 * n + 4]
            other_k = across_both(other_k, 0)
            both_k = (mine_k + other_k.astype(wide)).astype(low)
            arrived.append(
                ((across(both_k, offset),), (across_both(other_v, offset), across(mine_v, offset)))
            )
        own_k, own_v, *other = share(home_kept, home_got, [(wide, wide), (low,)])
        (other,) = other
        other = across_both(other, 0)
        own_k, own_v = own_k + other[0].astype(wide), own_v + other[1].astype(wide)
        for from_k, from_v in arrived:
            own_k = sum((a.astype(wide) for a in from_k), own_k)
            own_v = sum((a.astype(wide) for a in from_v), own_v)
    else:
        far = share(far_kept, far_got, [(low,)] * len(far_offsets))
        (own,) = share(home_kept, home_got, [(wide,)])
        for offset, array in zip(far_offsets, far):
            own = own + across(array, offset).astype(wide)
        own_k, own_v = (
            lax.psum_scatter(
                jnp.concatenate([own[t], own[2 + t]]), "head", scatter_dimension=0, tiled=True
            )
            for t in range(2)
        )
    grad_q = dq[0]
    for offset in q_units[1:]:
        grad_q = grad_q + across(dq[offset], offset).astype(jnp.float32)
    return (grad_q[None], own_k, own_v)


def solution(mesh):
    in_specs = (
        P("head", "blk", None),
        P("blk", None),
        P("blk", None),
        P("head", "blk", None),
        P("head", "blk", None),
        P("head", "blk"),
        P(),
    )
    out_specs = (P("head", "blk", None), P(("blk", "head"), None), P(("blk", "head"), None))

    def step(*args):
        return on_device(*args)

    step = jax.shard_map(
        step, mesh=mesh, in_specs=in_specs, out_specs=out_specs, check_vma=False
    )
    return step
```

```python
import functools

import jax
import jax.numpy as jnp
from jax import lax
from jax.experimental import pallas as pl
from jax.experimental.pallas import tpu as pltpu
from jax.sharding import PartitionSpec as P


LOG2E = 1.4426950408889634
WIDTH = 4
LIMIT = 24 * 2**20
VMEM = pl.BlockSpec(memory_space=pltpu.VMEM)
SMEM = pl.BlockSpec(memory_space=pltpu.SMEM)


def contract(left, right, dims):
    return lax.dot_general(left, right, (dims, ((), ())), preferred_element_type=jnp.float32)


def pieces_of(row):
    found = []
    for _ in range(3):
        piece = row.astype(jnp.bfloat16).astype(jnp.float32)
        found.append(piece)
        row = row - piece
    return found


def pack_kernel(split, *refs):
    given, (sent, kv_mine, kv_all), local, done = refs[:6], refs[6:9], refs[9:15], refs[15]
    copies = [pltpu.make_async_copy(a, b, done.at[n]) for n, (a, b) in enumerate(zip(given, local))]
    for copy in copies:
        copy.start()
    for copy in copies:
        copy.wait()
    k, v, q, g, o, low = local
    rows, width = q.shape
    block = rows // 2
    head = lax.axis_index("head")
    for part in range(2):
        half = lax.rem(head + part, 2) if split else part
        at = pl.ds(pl.multiple_of(half * block, block), block)
        kv_all[2 * part] = k[at, :]
        kv_all[2 * part + 1] = v[at, :]
        if part == 0:
            kv_mine[0] = k[at, :]
            kv_mine[1] = v[at, :]
    sent[:rows] = q[...]
    sent[rows : 2 * rows] = g[...]
    product = g[...].astype(jnp.float32) * o[...].astype(jnp.float32)
    delta = jnp.sum(product.T, axis=0, keepdims=True)
    lines = [
        piece[:, at : at + width]
        for row in (low[...] * LOG2E, delta)
        for piece in pieces_of(row)
        for at in range(0, rows, width)
    ]
    pad = sent.shape[0] - 2 * rows - len(lines)
    lines.append(jnp.zeros((pad, width), jnp.float32))
    sent[2 * rows :] = jnp.concatenate(lines, axis=0).astype(jnp.bfloat16)


def pack(query, output, out_grad, lse, key, value, split):
    rows, width = query.shape
    block = rows // 2
    lines = -(-6 * (rows // width) // 16) * 16
    given = (key, value, query, out_grad, output, lse)
    return pl.pallas_call(
        functools.partial(pack_kernel, split),
        out_shape=[
            jax.ShapeDtypeStruct((2 * rows + lines, width), jnp.bfloat16),
            jax.ShapeDtypeStruct((2, block, width), jnp.bfloat16),
            jax.ShapeDtypeStruct((4, block, width), jnp.bfloat16),
        ],
        in_specs=[pl.BlockSpec(memory_space=pltpu.HBM)] * len(given),
        out_specs=[VMEM] * 3,
        scratch_shapes=[pltpu.VMEM(a.shape, a.dtype) for a in given]
        + [pltpu.SemaphoreType.DMA((len(given),))],
        compiler_params=pltpu.CompilerParams(vmem_limit_bytes=LIMIT),
        name="pack",
    )(*[pltpu.with_memory_space_constraint(a, pltpu.HBM) for a in given])


def tile_kernel(shape, *refs):
    q_units, q_held, q_done, blocks, n_kv, k_held, k_done, skip, split, rows, width, scale = shape
    block = rows // 2
    n_q, n_k = 2 * len(q_units), len(blocks)
    refs = list(refs)

    def take(count):
        taken, refs[:] = refs[:count], refs[count:]
        return taken

    (order,) = take(1)
    q_in, kv_in = take(len(q_units)), take(n_kv)
    q_before = dict(zip(q_held, take(len(q_held))))
    k_before = take(1)[0] if k_held else None
    dq_out = dict(zip(q_units, take(len(q_units))))
    sent, kept = take(2) if k_done else (None, take(1)[0])
    q, g, low, delta, k, v, kt, dqt, total, q_at, k_at, pair_q, pair_k = refs

    me = lax.axis_index("blk")
    head = lax.axis_index("head")
    lines = rows // width
    for u, offset in enumerate(q_units):
        stats = q_in[u][2 * rows :].astype(jnp.float32)
        for half in range(2):
            i = 2 * u + half
            q[i] = q_in[u][half * block : (half + 1) * block]
            g[i] = q_in[u][rows + half * block : rows + (half + 1) * block]
            for kind, out in enumerate((low, delta)):
                pieces = [
                    stats[(3 * kind + p) * lines : (3 * kind + p + 1) * lines] for p in range(3)
                ]
                row = pieces[0] + pieces[1] + pieces[2]
                start = half * (lines // 2)
                out[i] = jnp.concatenate(
                    [row[c : c + 1] for c in range(start, start + lines // 2)], axis=1
                )
            q_at[i] = order[2 * (me ^ offset) + half]
            if offset in q_before:
                dqt[i] = q_before[offset][half]
            else:
                dqt[i] = jnp.zeros((width, block), jnp.float32)
    pieces = [(ref, at) for ref in kv_in for at in range(0, ref.shape[0], 2)]
    for j, ((ref, at), (offset, part)) in enumerate(zip(pieces, blocks)):
        k[j] = ref[at]
        v[j] = ref[at + 1]
        kt[j] = ref[at].T
        half = lax.rem(head + part, 2) if split else part
        k_at[j] = order[2 * (me ^ offset) + half]
        for t in range(2):
            if blocks[j] in k_held:
                total[2 * j + t] = k_before[2 * k_held.index(blocks[j]) + t]
            else:
                total[2 * j + t] = jnp.zeros((block, width), jnp.float32)

    found = jnp.int32(0)
    for i in range(n_q):
        at = q_at[i]
        for j in range(n_k):
            if (q_units[i // 2], blocks[j]) in skip:
                continue
            pair_q[found] = jnp.int32(i)
            pair_k[found] = jnp.int32(j)
            found += (at >= k_at[j]).astype(jnp.int32)
    for e in range(WIDTH - 1):
        pair_q[found + e] = jnp.int32(0)
        pair_k[found + e] = jnp.int32(-1)

    ahead = lax.broadcasted_iota(jnp.int32, (block, block), 1) - lax.broadcasted_iota(
        jnp.int32, (block, block), 0
    )

    def each_group(t, _):
        at_q = [pair_q[t * WIDTH + e] for e in range(WIDTH)]
        named = [pair_k[t * WIDTH + e] for e in range(WIDTH)]
        at_k = [jnp.maximum(j, 0) for j in named]

        def front(e):
            i, j = at_q[e], at_k[e]
            least = jnp.where(named[e] < 0, 2 * block, (k_at[j] - q_at[i]) * block)
            scores = contract(k[j], q[i], ((1,), (1,)))
            dprobs = contract(v[j], g[i], ((1,), (1,)))
            probs = jnp.where(ahead >= least, jnp.exp2(scores * (scale * LOG2E) - low[i]), 0.0)
            dscores = (probs * (dprobs - delta[i])).astype(jnp.bfloat16)
            return probs.astype(jnp.bfloat16), dscores

        ready = front(0)
        for e in range(WIDTH):
            probs_low, dscores = ready
            if e + 1 < WIDTH:
                ready = front(e + 1)
            i, j = at_q[e], at_k[e]
            total[2 * j + 1] += contract(probs_low, g[i], ((1,), (0,)))
            total[2 * j] += contract(dscores, q[i], ((1,), (0,)))
            dqt[i] += contract(kt[j], dscores, ((1,), (0,)))
        return 0

    lax.fori_loop(0, (found + WIDTH - 1) // WIDTH, each_group, 0)
    for u, offset in enumerate(q_units):
        out = dq_out[offset]
        for half in range(2):
            if offset in q_done:
                got = (dqt[2 * u + half] * scale).T.astype(out.dtype)
                out[half * block : (half + 1) * block] = got
            else:
                out[half] = dqt[2 * u + half]
    if k_done:
        place = {0: 0, 1: 0}
        for j, (offset, _) in enumerate(blocks):
            out, at = sent if offset & 1 else kept, place[offset & 1]
            out[at] = (total[2 * j] * scale).astype(out.dtype)
            out[at + 1] = total[2 * j + 1].astype(out.dtype)
            place[offset & 1] = at + 2
    else:
        kept[...] = total[...]


def blocks_of(kv):
    found = []
    for offset, arrays in kv.items():
        count = sum(a.shape[0] // 2 for a in arrays)
        found += [(offset, part) for part in range(count)]
    return tuple(found)


def tile_grads(
    order, q, kv, q_before, k_before, q_done, k_done, split, rows, scale, skip=frozenset()
):
    q_units, blocks = tuple(q), blocks_of(kv)
    kv = [a for arrays in kv.values() for a in arrays]
    width = kv[0].shape[2]
    block = rows // 2
    n_q, n_k = 2 * len(q_units), len(blocks)
    out_shape = []
    for offset in q_units:
        if offset not in q_done:
            out_shape.append(jax.ShapeDtypeStruct((2, width, block), jnp.float32))
        else:
            kind = jnp.bfloat16 if offset else jnp.float32
            out_shape.append(jax.ShapeDtypeStruct((rows, width), kind))
    if k_done:
        out_shape.append(jax.ShapeDtypeStruct((n_k, block, width), jnp.bfloat16))
        out_shape.append(jax.ShapeDtypeStruct((n_k, block, width), jnp.float32))
    else:
        out_shape.append(jax.ShapeDtypeStruct((2 * n_k, block, width), jnp.float32))
    pairs = n_q * n_k // 2
    q_held = tuple(o for o in q_units if o in q_before)
    k_held, k_before = k_before or ((), None)
    operands = [*q.values(), *kv, *(q_before[o] for o in q_held)] + ([k_before] if k_held else [])
    shape = (q_units, q_held, q_done, blocks, len(kv), k_held, k_done, skip, split, rows, width, scale)
    outs = pl.pallas_call(
        functools.partial(tile_kernel, shape),
        out_shape=out_shape,
        in_specs=[SMEM] + [VMEM] * len(operands),
        out_specs=[VMEM] * len(out_shape),
        scratch_shapes=[
            pltpu.VMEM((n_q, block, width), jnp.bfloat16),
            pltpu.VMEM((n_q, block, width), jnp.bfloat16),
            pltpu.VMEM((n_q, 1, block), jnp.float32),
            pltpu.VMEM((n_q, 1, block), jnp.float32),
            pltpu.VMEM((n_k, block, width), jnp.bfloat16),
            pltpu.VMEM((n_k, block, width), jnp.bfloat16),
            pltpu.VMEM((n_k, width, block), jnp.bfloat16),
            pltpu.VMEM((n_q, width, block), jnp.float32),
            pltpu.VMEM((2 * n_k, block, width), jnp.float32),
            pltpu.SMEM((n_q,), jnp.int32),
            pltpu.SMEM((n_k,), jnp.int32),
            pltpu.SMEM((n_q * n_k + WIDTH,), jnp.int32),
            pltpu.SMEM((n_q * n_k + WIDTH,), jnp.int32),
        ],
        cost_estimate=pl.CostEstimate(
            flops=pairs * block * block * width * 10,
            bytes_accessed=(n_q + n_k) * block * width * 8,
            transcendentals=pairs * block * block,
        ),
        compiler_params=pltpu.CompilerParams(vmem_limit_bytes=LIMIT),
        name="tile_grads",
    )(order, *operands)
    return dict(zip(q_units, outs)), outs[len(q_units) :]


def offsets_of(bits):
    found = [0]
    for bit in bits:
        found = found + [o | 1 << bit for o in found]
    return tuple(sorted(found))


def share_kernel(places, kept, got, *outs):
    for out, (at, size) in zip(outs, places):
        if size == 1:
            out[...] = (kept[at] + got[at].astype(jnp.float32)).astype(out.dtype)
        else:
            for n in range(size):
                out[n] = (kept[at + n] + got[at + n].astype(jnp.float32)).astype(out.dtype)


def share(kept, got, kinds):
    size = kept.shape[0] // len(kinds)
    places, shapes = [], []
    for n, group in enumerate(kinds):
        each = size // len(group)
        for e, kind in enumerate(group):
            places.append((n * size + e * each, each))
            lead = kept.shape[1:] if each == 1 else (each,) + kept.shape[1:]
            shapes.append(jax.ShapeDtypeStruct(lead, kind))
    return pl.pallas_call(
        functools.partial(share_kernel, tuple(places)),
        out_shape=shapes,
        in_specs=[VMEM] * 2,
        out_specs=[VMEM] * len(shapes),
        compiler_params=pltpu.CompilerParams(vmem_limit_bytes=LIMIT),
        name="share",
    )(kept, got)


def on_device(query, key, value, output, out_grad, lse, block_order):
    rows, width = key.shape
    scale = width ** (-0.5)
    devices = lax.axis_size("blk")
    heads = lax.axis_size("head")
    bits = devices.bit_length() - 1
    q_bits = tuple(range(bits))[1:3]
    k_bits = tuple(b for b in range(bits) if b not in q_bits)
    q_units, k_units = offsets_of(q_bits), offsets_of(k_bits)
    split = heads == 2

    def across(array, offset):
        return lax.ppermute(array, "blk", [(i, i ^ offset) for i in range(devices)])

    def across_both(array, offset):
        route = [(2 * i + h, 2 * (i ^ offset) + 1 - h) for i in range(devices) for h in range(2)]
        return lax.ppermute(array, ("blk", "head"), route)

    sent, kv_mine, kv_all = pack(query[0], output[0], out_grad[0], lse, key, value, split)

    held = {0: [kv_all]}
    for bit in k_bits[:0:-1]:
        for o in list(held):
            if split and o == 0:
                mine = across(kv_mine, 1 << bit)
                held[1 << bit] = [mine, across_both(mine, 0)]
            else:
                far = [across(a, 1 << bit) for a in held[o]]
                held[o | 1 << bit] = far
    q = {o: across(sent, o) if o else sent for o in q_units}
    for o in list(held):
        held[o | 1] = [across(a, 1) for a in held[o]]

    def some(array_of, units):
        return {o: array_of[o] for o in units}

    home = [o for o in k_units if o < 2]
    away = [o for o in k_units if o >= 2]
    mine, near, late = q_units[:1], q_units[1:-1], q_units[-1:]
    tile = functools.partial(tile_grads, block_order, split=split, rows=rows, scale=scale)
    home_kv, away_kv = some(held, home), some(held, away)
    home_blocks = blocks_of(home_kv)
    held_q, (total,) = tile(some(q, mine), home_kv, {}, None, (), False)
    if split:
        first_kv = {o: arrays[:1] for o, arrays in away_kv.items()}
        first = q_units[:2]
        first_blocks = blocks_of(first_kv)
        more_q, (away_total,) = tile(some(q, first), first_kv, held_q, None, (), False)
        held_q |= more_q
        away_before = (first_blocks, away_total)
        skip = frozenset((o, at) for o in first for at in first_blocks)
    else:
        away_before, skip = None, frozenset()
    more_q, (total,) = tile(
        some(q, near), home_kv, some(held_q, held_q.keys() & near), (home_blocks, total), (), False
    )
    held_q |= more_q
    dq, (far_sent, far_kept) = tile(
        some(q, q_units), away_kv, held_q, away_before, mine + near, True, skip=skip
    )
    held_q = some(dq, late)
    far_got = across(far_sent, 1)
    last_q, (home_sent, home_kept) = tile(
        some(q, late), home_kv, held_q, (home_blocks, total), late, True
    )
    dq |= last_q
    home_got = across(home_sent, 1)

    low, wide = jnp.bfloat16, jnp.float32
    far_offsets = [o for o in away if not o & 1]
    if split:
        far = share(far_kept, far_got, [(wide,), (low,)] * len(far_offsets))
        own, other = share(home_kept, home_got, [(wide,), (low,)])
        own = own + across_both(other, 0).astype(wide)
        for offset, kept, sent in zip(far_offsets, far[::2], far[1::2]):
            both = kept + across_both(sent, 0).astype(wide)
            own = own + across(both.astype(low), offset).astype(wide)
        own_k, own_v = own[0], own[1]
    else:
        far = share(far_kept, far_got, [(low,)] * len(far_offsets))
        (own,) = share(home_kept, home_got, [(wide,)])
        for offset, array in zip(far_offsets, far):
            own = own + across(array, offset).astype(wide)
        own_k, own_v = (
            lax.psum_scatter(
                jnp.concatenate([own[t], own[2 + t]]), "head", scatter_dimension=0, tiled=True
            )
            for t in range(2)
        )
    grad_q = dq[0]
    for offset in q_units[1:]:
        grad_q = grad_q + across(dq[offset], offset).astype(jnp.float32)
    return (grad_q[None], own_k, own_v)


def solution(mesh):
    in_specs = (
        P("head", "blk", None),
        P("blk", None),
        P("blk", None),
        P("head", "blk", None),
        P("head", "blk", None),
        P("head", "blk"),
        P(),
    )
    out_specs = (P("head", "blk", None), P(("blk", "head"), None), P(("blk", "head"), None))

    def step(*args):
        return on_device(*args)

    step = jax.shard_map(
        step, mesh=mesh, in_specs=in_specs, out_specs=out_specs, check_vma=False
    )
    return step
```

```python
import functools

import jax
import jax.numpy as jnp
from jax import lax
from jax.experimental import pallas as pl
from jax.experimental.pallas import tpu as pltpu
from jax.sharding import PartitionSpec as P


LOG2E = 1.4426950408889634
WIDTH = 4
LIMIT = 24 * 2**20
VMEM = pl.BlockSpec(memory_space=pltpu.VMEM)


def contract(left, right, dims):
    return lax.dot_general(left, right, (dims, ((), ())), preferred_element_type=jnp.float32)


def pieces_of(row):
    found = []
    for _ in range(3):
        piece = row.astype(jnp.bfloat16).astype(jnp.float32)
        found.append(piece)
        row = row - piece
    return found


def pack_kernel(split, *refs):
    given, (sent, kv_mine, kv_all), local, done = refs[:6], refs[6:9], refs[9:15], refs[15]
    copies = [pltpu.make_async_copy(a, b, done.at[n]) for n, (a, b) in enumerate(zip(given, local))]
    for copy in copies:
        copy.start()
    for copy in copies:
        copy.wait()
    k, v, q, g, o, low = local
    rows, width = q.shape
    block = rows // 2
    head = lax.axis_index("head")
    for part in range(2):
        half = lax.rem(head + part, 2) if split else part
        at = pl.ds(pl.multiple_of(half * block, block), block)
        kv_all[2 * part] = k[at, :]
        kv_all[2 * part + 1] = v[at, :]
        if part == 0:
            kv_mine[0] = k[at, :]
            kv_mine[1] = v[at, :]
    sent[:rows] = q[...]
    sent[rows : 2 * rows] = g[...]
    product = g[...].astype(jnp.float32) * o[...].astype(jnp.float32)
    delta = jnp.sum(product.T, axis=0, keepdims=True)
    lines = [
        piece[:, at : at + width]
        for row in (low[...] * LOG2E, delta)
        for piece in pieces_of(row)
        for at in range(0, rows, width)
    ]
    pad = sent.shape[0] - 2 * rows - len(lines)
    lines.append(jnp.zeros((pad, width), jnp.float32))
    sent[2 * rows :] = jnp.concatenate(lines, axis=0).astype(jnp.bfloat16)


def pack(query, output, out_grad, lse, key, value, split):
    rows, width = query.shape
    block = rows // 2
    lines = -(-6 * (rows // width) // 16) * 16
    given = (key, value, query, out_grad, output, lse)
    return pl.pallas_call(
        functools.partial(pack_kernel, split),
        out_shape=[
            jax.ShapeDtypeStruct((2 * rows + lines, width), jnp.bfloat16),
            jax.ShapeDtypeStruct((2, block, width), jnp.bfloat16),
            jax.ShapeDtypeStruct((4, block, width), jnp.bfloat16),
        ],
        in_specs=[pl.BlockSpec(memory_space=pltpu.HBM)] * len(given),
        out_specs=[VMEM] * 3,
        scratch_shapes=[pltpu.VMEM(a.shape, a.dtype) for a in given]
        + [pltpu.SemaphoreType.DMA((len(given),))],
        compiler_params=pltpu.CompilerParams(vmem_limit_bytes=LIMIT),
        name="pack",
    )(*[pltpu.with_memory_space_constraint(a, pltpu.HBM) for a in given])


def tile_kernel(shape, *refs):
    q_units, q_held, q_done, blocks, n_kv, k_held, k_done, skip, split, rows, width, scale = shape
    block = rows // 2
    n_q, n_k = 2 * len(q_units), len(blocks)
    refs = list(refs)

    def take(count):
        taken, refs[:] = refs[:count], refs[count:]
        return taken

    (order,) = take(1)
    q_in, kv_in = take(len(q_units)), take(n_kv)
    q_before = dict(zip(q_held, take(len(q_held))))
    k_before = take(1)[0] if k_held else None
    dq_out = dict(zip(q_units, take(len(q_units))))
    sent, kept = take(2) if k_done else (None, take(1)[0])
    q, g, low, delta, k, v, kt, dqt, total, q_at, k_at, pair_q, pair_k = refs

    me = lax.axis_index("blk")
    head = lax.axis_index("head")
    lines = rows // width
    lane = lax.broadcasted_iota(jnp.int32, order.shape, 1)

    def place(block_index):
        return jnp.sum(jnp.where(lane == block_index, order[...], 0.0)).astype(jnp.int32)

    for u, offset in enumerate(q_units):
        stats = q_in[u][2 * rows :].astype(jnp.float32)
        for half in range(2):
            i = 2 * u + half
            q[i] = q_in[u][half * block : (half + 1) * block]
            g[i] = q_in[u][rows + half * block : rows + (half + 1) * block]
            for kind, out in enumerate((low, delta)):
                pieces = [
                    stats[(3 * kind + p) * lines : (3 * kind + p + 1) * lines] for p in range(3)
                ]
                row = pieces[0] + pieces[1] + pieces[2]
                start = half * (lines // 2)
                out[i] = jnp.concatenate(
                    [row[c : c + 1] for c in range(start, start + lines // 2)], axis=1
                )
            q_at[i] = place(2 * (me ^ offset) + half)
            if offset in q_before:
                dqt[i] = q_before[offset][half]
            else:
                dqt[i] = jnp.zeros((width, block), jnp.float32)
    pieces = [(ref, at) for ref in kv_in for at in range(0, ref.shape[0], 2)]
    for j, ((ref, at), (offset, part)) in enumerate(zip(pieces, blocks)):
        k[j] = ref[at]
        v[j] = ref[at + 1]
        kt[j] = ref[at].T
        half = lax.rem(head + part, 2) if split else part
        k_at[j] = place(2 * (me ^ offset) + half)
        for t in range(2):
            if blocks[j] in k_held:
                total[2 * j + t] = k_before[2 * k_held.index(blocks[j]) + t]
            else:
                total[2 * j + t] = jnp.zeros((block, width), jnp.float32)

    found = jnp.int32(0)
    for i in range(n_q):
        at = q_at[i]
        for j in range(n_k):
            if (q_units[i // 2], blocks[j]) in skip:
                continue
            pair_q[found] = jnp.int32(i)
            pair_k[found] = jnp.int32(j)
            found += (at >= k_at[j]).astype(jnp.int32)
    for e in range(WIDTH - 1):
        pair_q[found + e] = jnp.int32(0)
        pair_k[found + e] = jnp.int32(-1)

    ahead = lax.broadcasted_iota(jnp.int32, (block, block), 1) - lax.broadcasted_iota(
        jnp.int32, (block, block), 0
    )

    def each_group(t, _):
        at_q = [pair_q[t * WIDTH + e] for e in range(WIDTH)]
        named = [pair_k[t * WIDTH + e] for e in range(WIDTH)]
        at_k = [jnp.maximum(j, 0) for j in named]

        def front(e):
            i, j = at_q[e], at_k[e]
            least = jnp.where(named[e] < 0, 2 * block, (k_at[j] - q_at[i]) * block)
            scores = contract(k[j], q[i], ((1,), (1,)))
            dprobs = contract(v[j], g[i], ((1,), (1,)))
            probs = jnp.where(ahead >= least, jnp.exp2(scores * (scale * LOG2E) - low[i]), 0.0)
            dscores = (probs * (dprobs - delta[i])).astype(jnp.bfloat16)
            return probs.astype(jnp.bfloat16), dscores

        ready = front(0)
        for e in range(WIDTH):
            probs_low, dscores = ready
            if e + 1 < WIDTH:
                ready = front(e + 1)
            i, j = at_q[e], at_k[e]
            total[2 * j + 1] += contract(probs_low, g[i], ((1,), (0,)))
            total[2 * j] += contract(dscores, q[i], ((1,), (0,)))
            dqt[i] += contract(kt[j], dscores, ((1,), (0,)))
        return 0

    lax.fori_loop(0, (found + WIDTH - 1) // WIDTH, each_group, 0)
    for u, offset in enumerate(q_units):
        out = dq_out[offset]
        for half in range(2):
            if offset in q_done:
                got = (dqt[2 * u + half] * scale).T.astype(out.dtype)
                out[half * block : (half + 1) * block] = got
            else:
                out[half] = dqt[2 * u + half]
    if k_done:
        place = {0: 0, 1: 0}
        for j, (offset, _) in enumerate(blocks):
            out, at = sent if offset & 1 else kept, place[offset & 1]
            out[at] = (total[2 * j] * scale).astype(out.dtype)
            out[at + 1] = total[2 * j + 1].astype(out.dtype)
            place[offset & 1] = at + 2
    else:
        kept[...] = total[...]


def blocks_of(kv):
    found = []
    for offset, arrays in kv.items():
        count = sum(a.shape[0] // 2 for a in arrays)
        found += [(offset, part) for part in range(count)]
    return tuple(found)


def tile_grads(
    order, q, kv, q_before, k_before, q_done, k_done, split, rows, scale, skip=frozenset()
):
    q_units, blocks = tuple(q), blocks_of(kv)
    kv = [a for arrays in kv.values() for a in arrays]
    width = kv[0].shape[2]
    block = rows // 2
    n_q, n_k = 2 * len(q_units), len(blocks)
    out_shape = []
    for offset in q_units:
        if offset not in q_done:
            out_shape.append(jax.ShapeDtypeStruct((2, width, block), jnp.float32))
        else:
            kind = jnp.bfloat16 if offset else jnp.float32
            out_shape.append(jax.ShapeDtypeStruct((rows, width), kind))
    if k_done:
        out_shape.append(jax.ShapeDtypeStruct((n_k, block, width), jnp.bfloat16))
        out_shape.append(jax.ShapeDtypeStruct((n_k, block, width), jnp.float32))
    else:
        out_shape.append(jax.ShapeDtypeStruct((2 * n_k, block, width), jnp.float32))
    pairs = n_q * n_k // 2
    q_held = tuple(o for o in q_units if o in q_before)
    k_held, k_before = k_before or ((), None)
    operands = [*q.values(), *kv, *(q_before[o] for o in q_held)] + ([k_before] if k_held else [])
    shape = (q_units, q_held, q_done, blocks, len(kv), k_held, k_done, skip, split, rows, width, scale)
    outs = pl.pallas_call(
        functools.partial(tile_kernel, shape),
        out_shape=out_shape,
        in_specs=[VMEM] * (1 + len(operands)),
        out_specs=[VMEM] * len(out_shape),
        scratch_shapes=[
            pltpu.VMEM((n_q, block, width), jnp.bfloat16),
            pltpu.VMEM((n_q, block, width), jnp.bfloat16),
            pltpu.VMEM((n_q, 1, block), jnp.float32),
            pltpu.VMEM((n_q, 1, block), jnp.float32),
            pltpu.VMEM((n_k, block, width), jnp.bfloat16),
            pltpu.VMEM((n_k, block, width), jnp.bfloat16),
            pltpu.VMEM((n_k, width, block), jnp.bfloat16),
            pltpu.VMEM((n_q, width, block), jnp.float32),
            pltpu.VMEM((2 * n_k, block, width), jnp.float32),
            pltpu.SMEM((n_q,), jnp.int32),
            pltpu.SMEM((n_k,), jnp.int32),
            pltpu.SMEM((n_q * n_k + WIDTH,), jnp.int32),
            pltpu.SMEM((n_q * n_k + WIDTH,), jnp.int32),
        ],
        cost_estimate=pl.CostEstimate(
            flops=pairs * block * block * width * 10,
            bytes_accessed=(n_q + n_k) * block * width * 8,
            transcendentals=pairs * block * block,
        ),
        compiler_params=pltpu.CompilerParams(vmem_limit_bytes=LIMIT),
        name="tile_grads",
    )(order, *operands)
    return dict(zip(q_units, outs)), outs[len(q_units) :]


def offsets_of(bits):
    found = [0]
    for bit in bits:
        found = found + [o | 1 << bit for o in found]
    return tuple(sorted(found))


def share_kernel(places, kept, got, *outs):
    for out, (at, size) in zip(outs, places):
        if size == 1:
            out[...] = (kept[at] + got[at].astype(jnp.float32)).astype(out.dtype)
        else:
            for n in range(size):
                out[n] = (kept[at + n] + got[at + n].astype(jnp.float32)).astype(out.dtype)


def share(kept, got, kinds):
    size = kept.shape[0] // len(kinds)
    places, shapes = [], []
    for n, group in enumerate(kinds):
        each = size // len(group)
        for e, kind in enumerate(group):
            places.append((n * size + e * each, each))
            lead = kept.shape[1:] if each == 1 else (each,) + kept.shape[1:]
            shapes.append(jax.ShapeDtypeStruct(lead, kind))
    return pl.pallas_call(
        functools.partial(share_kernel, tuple(places)),
        out_shape=shapes,
        in_specs=[VMEM] * 2,
        out_specs=[VMEM] * len(shapes),
        compiler_params=pltpu.CompilerParams(vmem_limit_bytes=LIMIT),
        name="share",
    )(kept, got)


def on_device(query, key, value, output, out_grad, lse, block_order):
    rows, width = key.shape
    scale = width ** (-0.5)
    devices = lax.axis_size("blk")
    heads = lax.axis_size("head")
    bits = devices.bit_length() - 1
    q_bits = tuple(range(bits))[1:3]
    k_bits = tuple(b for b in range(bits) if b not in q_bits)
    q_units, k_units = offsets_of(q_bits), offsets_of(k_bits)
    split = heads == 2

    def across(array, offset):
        return lax.ppermute(array, "blk", [(i, i ^ offset) for i in range(devices)])

    def across_both(array, offset):
        route = [(2 * i + h, 2 * (i ^ offset) + 1 - h) for i in range(devices) for h in range(2)]
        return lax.ppermute(array, ("blk", "head"), route)

    sent, kv_mine, kv_all = pack(query[0], output[0], out_grad[0], lse, key, value, split)

    held = {0: [kv_all]}
    for bit in k_bits[:0:-1]:
        for o in list(held):
            if split and o == 0:
                mine = across(kv_mine, 1 << bit)
                held[1 << bit] = [mine, across_both(mine, 0)]
            else:
                far = [across(a, 1 << bit) for a in held[o]]
                held[o | 1 << bit] = far
    q = {o: across(sent, o) if o else sent for o in q_units}
    for o in list(held):
        held[o | 1] = [across(a, 1) for a in held[o]]

    def some(array_of, units):
        return {o: array_of[o] for o in units}

    home = [o for o in k_units if o < 2]
    away = [o for o in k_units if o >= 2]
    mine, near, late = q_units[:1], q_units[1:-1], q_units[-1:]
    order = block_order.astype(jnp.float32)[None]
    tile = functools.partial(tile_grads, order, split=split, rows=rows, scale=scale)
    home_kv, away_kv = some(held, home), some(held, away)
    home_blocks = blocks_of(home_kv)
    held_q, (total,) = tile(some(q, mine), home_kv, {}, None, (), False)
    if split:
        first_kv = {o: arrays[:1] for o, arrays in away_kv.items()}
        first = q_units[:2]
        first_blocks = blocks_of(first_kv)
        more_q, (away_total,) = tile(some(q, first), first_kv, held_q, None, (), False)
        held_q |= more_q
        away_before = (first_blocks, away_total)
        skip = frozenset((o, at) for o in first for at in first_blocks)
    else:
        away_before, skip = None, frozenset()
    more_q, (total,) = tile(
        some(q, near), home_kv, some(held_q, held_q.keys() & near), (home_blocks, total), (), False
    )
    held_q |= more_q
    dq, (far_sent, far_kept) = tile(
        some(q, q_units), away_kv, held_q, away_before, mine + near, True, skip=skip
    )
    held_q = some(dq, late)
    far_got = across(far_sent, 1)
    last_q, (home_sent, home_kept) = tile(
        some(q, late), home_kv, held_q, (home_blocks, total), late, True
    )
    dq |= last_q
    home_got = across(home_sent, 1)

    low, wide = jnp.bfloat16, jnp.float32
    far_offsets = [o for o in away if not o & 1]
    if split:
        far = share(far_kept, far_got, [(wide,), (low,)] * len(far_offsets))
        own, other = share(home_kept, home_got, [(wide,), (low,)])
        own = own + across_both(other, 0).astype(wide)
        for offset, kept, sent in zip(far_offsets, far[::2], far[1::2]):
            both = kept + across_both(sent, 0).astype(wide)
            own = own + across(both.astype(low), offset).astype(wide)
        own_k, own_v = own[0], own[1]
    else:
        far = share(far_kept, far_got, [(low,)] * len(far_offsets))
        (own,) = share(home_kept, home_got, [(wide,)])
        for offset, array in zip(far_offsets, far):
            own = own + across(array, offset).astype(wide)
        own_k, own_v = (
            lax.psum_scatter(
                jnp.concatenate([own[t], own[2 + t]]), "head", scatter_dimension=0, tiled=True
            )
            for t in range(2)
        )
    grad_q = dq[0]
    for offset in q_units[1:]:
        grad_q = grad_q + across(dq[offset], offset).astype(jnp.float32)
    return (grad_q[None], own_k, own_v)


def solution(mesh):
    in_specs = (
        P("head", "blk", None),
        P("blk", None),
        P("blk", None),
        P("head", "blk", None),
        P("head", "blk", None),
        P("head", "blk"),
        P(),
    )
    out_specs = (P("head", "blk", None), P(("blk", "head"), None), P(("blk", "head"), None))

    def step(*args):
        return on_device(*args)

    step = jax.shard_map(
        step, mesh=mesh, in_specs=in_specs, out_specs=out_specs, check_vma=False
    )
    return step
```

```python
import functools

import jax
import jax.numpy as jnp
from jax import lax
from jax.experimental import pallas as pl
from jax.experimental.pallas import tpu as pltpu
from jax.sharding import PartitionSpec as P


LOG2E = 1.4426950408889634
WIDTH = 4
LIMIT = 24 * 2**20
VMEM = pl.BlockSpec(memory_space=pltpu.VMEM)


def contract(left, right, dims):
    return lax.dot_general(left, right, (dims, ((), ())), preferred_element_type=jnp.float32)


def pieces_of(row):
    found = []
    for _ in range(3):
        piece = row.astype(jnp.bfloat16).astype(jnp.float32)
        found.append(piece)
        row = row - piece
    return found


def pack_kernel(split, *refs):
    given, (sent, kv_mine, kv_all), local, done = refs[:6], refs[6:9], refs[9:15], refs[15]
    copies = [pltpu.make_async_copy(a, b, done.at[n]) for n, (a, b) in enumerate(zip(given, local))]
    for copy in copies:
        copy.start()
    for copy in copies:
        copy.wait()
    k, v, q, g, o, low = local
    rows, width = q.shape
    block = rows // 2
    head = lax.axis_index("head")
    for part in range(2):
        half = lax.rem(head + part, 2) if split else part
        at = pl.ds(pl.multiple_of(half * block, block), block)
        kv_all[2 * part] = k[at, :]
        kv_all[2 * part + 1] = v[at, :]
        if part == 0:
            kv_mine[0] = k[at, :]
            kv_mine[1] = v[at, :]
    sent[:rows] = q[...]
    sent[rows : 2 * rows] = g[...]
    product = g[...].astype(jnp.float32) * o[...].astype(jnp.float32)
    delta = jnp.sum(product.T, axis=0, keepdims=True)
    lines = [
        piece[:, at : at + width]
        for row in (low[...] * LOG2E, delta)
        for piece in pieces_of(row)
        for at in range(0, rows, width)
    ]
    pad = sent.shape[0] - 2 * rows - len(lines)
    lines.append(jnp.zeros((pad, width), jnp.float32))
    sent[2 * rows :] = jnp.concatenate(lines, axis=0).astype(jnp.bfloat16)


def pack(query, output, out_grad, lse, key, value, split):
    rows, width = query.shape
    block = rows // 2
    lines = -(-6 * (rows // width) // 16) * 16
    given = (key, value, query, out_grad, output, lse)
    return pl.pallas_call(
        functools.partial(pack_kernel, split),
        out_shape=[
            jax.ShapeDtypeStruct((2 * rows + lines, width), jnp.bfloat16),
            jax.ShapeDtypeStruct((2, block, width), jnp.bfloat16),
            jax.ShapeDtypeStruct((4, block, width), jnp.bfloat16),
        ],
        in_specs=[pl.BlockSpec(memory_space=pltpu.HBM)] * len(given),
        out_specs=[VMEM] * 3,
        scratch_shapes=[pltpu.VMEM(a.shape, a.dtype) for a in given]
        + [pltpu.SemaphoreType.DMA((len(given),))],
        compiler_params=pltpu.CompilerParams(vmem_limit_bytes=LIMIT),
        name="pack",
    )(*[pltpu.with_memory_space_constraint(a, pltpu.HBM) for a in given])


def tile_kernel(shape, *refs):
    q_units, q_held, q_done, blocks, n_kv, k_held, k_done, skip, split, rows, width, scale = shape
    block = rows // 2
    n_q, n_k = 2 * len(q_units), len(blocks)
    refs = list(refs)

    def take(count):
        taken, refs[:] = refs[:count], refs[count:]
        return taken

    (order,) = take(1)
    q_in, kv_in = take(len(q_units)), take(n_kv)
    q_before = dict(zip(q_held, take(len(q_held))))
    k_before = take(len(k_held))
    dq_out = dict(zip(q_units, take(len(q_units))))
    sent, kept = take(2) if k_done else (None, take(1)[0])
    q, g, low, delta, k, v, kt, dqt, *scratch, q_at, k_at, pair_q, pair_k = refs

    me = lax.axis_index("blk")
    head = lax.axis_index("head")
    total = scratch[0] if k_done else kept
    held_at = {at: (ref, n) for ref, ids in zip(k_before, k_held) for n, at in enumerate(ids)}
    lines = rows // width
    lane = lax.broadcasted_iota(jnp.int32, order.shape, 1)

    def place(block_index):
        return jnp.sum(jnp.where(lane == block_index, order[...], 0.0)).astype(jnp.int32)

    for u, offset in enumerate(q_units):
        stats = q_in[u][2 * rows :].astype(jnp.float32)
        for half in range(2):
            i = 2 * u + half
            q[i] = q_in[u][half * block : (half + 1) * block]
            g[i] = q_in[u][rows + half * block : rows + (half + 1) * block]
            for kind, out in enumerate((low, delta)):
                pieces = [
                    stats[(3 * kind + p) * lines : (3 * kind + p + 1) * lines] for p in range(3)
                ]
                row = pieces[0] + pieces[1] + pieces[2]
                start = half * (lines // 2)
                out[i] = jnp.concatenate(
                    [row[c : c + 1] for c in range(start, start + lines // 2)], axis=1
                )
            q_at[i] = place(2 * (me ^ offset) + half)
            if offset in q_before:
                dqt[i] = q_before[offset][half]
            else:
                dqt[i] = jnp.zeros((width, block), jnp.float32)
    pieces = [(ref, at) for ref in kv_in for at in range(0, ref.shape[0], 2)]
    for j, ((ref, at), (offset, part)) in enumerate(zip(pieces, blocks)):
        k[j] = ref[at]
        v[j] = ref[at + 1]
        kt[j] = ref[at].T
        half = lax.rem(head + part, 2) if split else part
        k_at[j] = place(2 * (me ^ offset) + half)
        for t in range(2):
            if blocks[j] in held_at:
                from_ref, n = held_at[blocks[j]]
                total[2 * j + t] = from_ref[2 * n + t]
            else:
                total[2 * j + t] = jnp.zeros((block, width), jnp.float32)

    found = jnp.int32(0)
    for i in range(n_q):
        at = q_at[i]
        for j in range(n_k):
            if (q_units[i // 2], blocks[j]) in skip:
                continue
            pair_q[found] = jnp.int32(i)
            pair_k[found] = jnp.int32(j)
            found += (at >= k_at[j]).astype(jnp.int32)
    for e in range(WIDTH - 1):
        pair_q[found + e] = jnp.int32(0)
        pair_k[found + e] = jnp.int32(-1)

    ahead = lax.broadcasted_iota(jnp.int32, (block, block), 1) - lax.broadcasted_iota(
        jnp.int32, (block, block), 0
    )

    def each_group(t, _):
        at_q = [pair_q[t * WIDTH + e] for e in range(WIDTH)]
        named = [pair_k[t * WIDTH + e] for e in range(WIDTH)]
        at_k = [jnp.maximum(j, 0) for j in named]

        def front(e):
            i, j = at_q[e], at_k[e]
            least = jnp.where(named[e] < 0, 2 * block, (k_at[j] - q_at[i]) * block)
            scores = contract(k[j], q[i], ((1,), (1,)))
            dprobs = contract(v[j], g[i], ((1,), (1,)))
            probs = jnp.where(ahead >= least, jnp.exp2(scores * (scale * LOG2E) - low[i]), 0.0)
            dscores = (probs * (dprobs - delta[i])).astype(jnp.bfloat16)
            return probs.astype(jnp.bfloat16), dscores

        ready = front(0)
        for e in range(WIDTH):
            probs_low, dscores = ready
            if e + 1 < WIDTH:
                ready = front(e + 1)
            i, j = at_q[e], at_k[e]
            total[2 * j + 1] += contract(probs_low, g[i], ((1,), (0,)))
            total[2 * j] += contract(dscores, q[i], ((1,), (0,)))
            dqt[i] += contract(kt[j], dscores, ((1,), (0,)))
        return 0

    lax.fori_loop(0, (found + WIDTH - 1) // WIDTH, each_group, 0)
    for u, offset in enumerate(q_units):
        out = dq_out[offset]
        for half in range(2):
            if offset in q_done:
                got = (dqt[2 * u + half] * scale).T.astype(out.dtype)
                out[half * block : (half + 1) * block] = got
            else:
                out[half] = dqt[2 * u + half]
    if k_done:
        place = {0: 0, 1: 0}
        for j, (offset, _) in enumerate(blocks):
            out, at = sent if offset & 1 else kept, place[offset & 1]
            out[at] = (total[2 * j] * scale).astype(out.dtype)
            out[at + 1] = total[2 * j + 1].astype(out.dtype)
            place[offset & 1] = at + 2


def blocks_of(kv):
    found = []
    for offset, arrays in kv.items():
        count = sum(a.shape[0] // 2 for a in arrays)
        found += [(offset, part) for part in range(count)]
    return tuple(found)


def tile_grads(
    order, q, kv, q_before, k_before, q_done, k_done, split, rows, scale, skip=frozenset()
):
    q_units, blocks = tuple(q), blocks_of(kv)
    kv = [a for arrays in kv.values() for a in arrays]
    width = kv[0].shape[2]
    block = rows // 2
    n_q, n_k = 2 * len(q_units), len(blocks)
    out_shape = []
    for offset in q_units:
        if offset not in q_done:
            out_shape.append(jax.ShapeDtypeStruct((2, width, block), jnp.float32))
        else:
            kind = jnp.bfloat16 if offset else jnp.float32
            out_shape.append(jax.ShapeDtypeStruct((rows, width), kind))
    if k_done:
        out_shape.append(jax.ShapeDtypeStruct((n_k, block, width), jnp.bfloat16))
        out_shape.append(jax.ShapeDtypeStruct((n_k, block, width), jnp.float32))
    else:
        out_shape.append(jax.ShapeDtypeStruct((2 * n_k, block, width), jnp.float32))
    pairs = n_q * n_k // 2
    q_held = tuple(o for o in q_units if o in q_before)
    k_held = tuple(ids for ids, _ in k_before)
    operands = [*q.values(), *kv, *(q_before[o] for o in q_held), *(a for _, a in k_before)]
    shape = (q_units, q_held, q_done, blocks, len(kv), k_held, k_done, skip, split, rows, width, scale)
    outs = pl.pallas_call(
        functools.partial(tile_kernel, shape),
        out_shape=out_shape,
        in_specs=[VMEM] * (1 + len(operands)),
        out_specs=[VMEM] * len(out_shape),
        scratch_shapes=[
            pltpu.VMEM((n_q, block, width), jnp.bfloat16),
            pltpu.VMEM((n_q, block, width), jnp.bfloat16),
            pltpu.VMEM((n_q, 1, block), jnp.float32),
            pltpu.VMEM((n_q, 1, block), jnp.float32),
            pltpu.VMEM((n_k, block, width), jnp.bfloat16),
            pltpu.VMEM((n_k, block, width), jnp.bfloat16),
            pltpu.VMEM((n_k, width, block), jnp.bfloat16),
            pltpu.VMEM((n_q, width, block), jnp.float32),
            *[pltpu.VMEM((2 * n_k, block, width), jnp.float32)] * k_done,
            pltpu.SMEM((n_q,), jnp.int32),
            pltpu.SMEM((n_k,), jnp.int32),
            pltpu.SMEM((n_q * n_k + WIDTH,), jnp.int32),
            pltpu.SMEM((n_q * n_k + WIDTH,), jnp.int32),
        ],
        cost_estimate=pl.CostEstimate(
            flops=pairs * block * block * width * 10,
            bytes_accessed=(n_q + n_k) * block * width * 8,
            transcendentals=pairs * block * block,
        ),
        compiler_params=pltpu.CompilerParams(vmem_limit_bytes=LIMIT),
        name="tile_grads",
    )(order, *operands)
    return dict(zip(q_units, outs)), outs[len(q_units) :]


def offsets_of(bits):
    found = [0]
    for bit in bits:
        found = found + [o | 1 << bit for o in found]
    return tuple(sorted(found))


def share_kernel(places, kept, got, *outs):
    for out, (at, size) in zip(outs, places):
        if size == 1:
            out[...] = (kept[at] + got[at].astype(jnp.float32)).astype(out.dtype)
        else:
            for n in range(size):
                out[n] = (kept[at + n] + got[at + n].astype(jnp.float32)).astype(out.dtype)


def share(kept, got, kinds):
    size = kept.shape[0] // len(kinds)
    places, shapes = [], []
    for n, group in enumerate(kinds):
        each = size // len(group)
        for e, kind in enumerate(group):
            places.append((n * size + e * each, each))
            lead = kept.shape[1:] if each == 1 else (each,) + kept.shape[1:]
            shapes.append(jax.ShapeDtypeStruct(lead, kind))
    return pl.pallas_call(
        functools.partial(share_kernel, tuple(places)),
        out_shape=shapes,
        in_specs=[VMEM] * 2,
        out_specs=[VMEM] * len(shapes),
        compiler_params=pltpu.CompilerParams(vmem_limit_bytes=LIMIT),
        name="share",
    )(kept, got)


def on_device(query, key, value, output, out_grad, lse, block_order):
    rows, width = key.shape
    scale = width ** (-0.5)
    devices = lax.axis_size("blk")
    heads = lax.axis_size("head")
    bits = devices.bit_length() - 1
    q_bits = tuple(range(bits))[1:3]
    k_bits = tuple(b for b in range(bits) if b not in q_bits)
    q_units, k_units = offsets_of(q_bits), offsets_of(k_bits)
    split = heads == 2

    def across(array, offset):
        return lax.ppermute(array, "blk", [(i, i ^ offset) for i in range(devices)])

    def across_both(array, offset):
        route = [(2 * i + h, 2 * (i ^ offset) + 1 - h) for i in range(devices) for h in range(2)]
        return lax.ppermute(array, ("blk", "head"), route)

    sent, kv_mine, kv_all = pack(query[0], output[0], out_grad[0], lse, key, value, split)

    held = {0: [kv_all]}
    for bit in k_bits[:0:-1]:
        for o in list(held):
            if split and o == 0:
                mine = across(kv_mine, 1 << bit)
                held[1 << bit] = [mine, across_both(mine, 0)]
            else:
                far = [across(a, 1 << bit) for a in held[o]]
                held[o | 1 << bit] = far
    q = {o: across(sent, o) if o else sent for o in q_units}
    for o in list(held):
        held[o | 1] = [across(a, 1) for a in held[o]]

    def some(array_of, units):
        return {o: array_of[o] for o in units}

    home = [o for o in k_units if o < 2]
    away = [o for o in k_units if o >= 2]
    mine, near, late = q_units[:1], q_units[1:-1], q_units[-1:]
    order = block_order.astype(jnp.float32)[None]
    tile = functools.partial(tile_grads, order, split=split, rows=rows, scale=scale)
    home_kv, away_kv = some(held, home), some(held, away)
    home_blocks = blocks_of(home_kv)
    held_q, (total,) = tile(some(q, mine), home_kv, {}, (), (), False)
    before, skip = [(home_blocks, total)], frozenset()
    near_kv, near_skip = home_kv, frozenset()
    if split:
        first_kv = {o: arrays[:1] for o, arrays in away_kv.items()}
        first, first_blocks = q_units[:2], blocks_of(first_kv)
        more_q, (total,) = tile(some(q, first), first_kv, held_q, (), (), False)
        held_q |= more_q
        before.append((first_blocks, total))
        near_kv = home_kv | first_kv
        near_skip = frozenset((o, at) for o in near[:1] for at in first_blocks)
        skip = frozenset((o, at) for o in mine + near for at in first_blocks)
    more_q, (total,) = tile(
        some(q, near),
        near_kv,
        some(held_q, held_q.keys() & near),
        before,
        (),
        False,
        skip=near_skip,
    )
    held_q |= more_q
    before = [(blocks_of(near_kv), total)]
    dq, (far_sent, far_kept) = tile(
        some(q, q_units), away_kv, held_q, before, mine + near, True, skip=skip
    )
    held_q = some(dq, late)
    far_got = across(far_sent, 1)
    last_q, (home_sent, home_kept) = tile(some(q, late), home_kv, held_q, before, late, True)
    dq |= last_q
    home_got = across(home_sent, 1)

    low, wide = jnp.bfloat16, jnp.float32
    far_offsets = [o for o in away if not o & 1]
    if split:
        far = share(far_kept, far_got, [(wide,), (low,)] * len(far_offsets))
        own, other = share(home_kept, home_got, [(wide,), (low,)])
        own = own + across_both(other, 0).astype(wide)
        for offset, kept, sent in zip(far_offsets, far[::2], far[1::2]):
            both = kept + across_both(sent, 0).astype(wide)
            own = own + across(both.astype(low), offset).astype(wide)
        own_k, own_v = own[0], own[1]
    else:
        far = share(far_kept, far_got, [(low,)] * len(far_offsets))
        (own,) = share(home_kept, home_got, [(wide,)])
        for offset, array in zip(far_offsets, far):
            own = own + across(array, offset).astype(wide)
        own_k, own_v = (
            lax.psum_scatter(
                jnp.concatenate([own[t], own[2 + t]]), "head", scatter_dimension=0, tiled=True
            )
            for t in range(2)
        )
    grad_q = dq[0]
    for offset in q_units[1:]:
        grad_q = grad_q + across(dq[offset], offset).astype(jnp.float32)
    return (grad_q[None], own_k, own_v)


def solution(mesh):
    in_specs = (
        P("head", "blk", None),
        P("blk", None),
        P("blk", None),
        P("head", "blk", None),
        P("head", "blk", None),
        P("head", "blk"),
        P(),
    )
    out_specs = (P("head", "blk", None), P(("blk", "head"), None), P(("blk", "head"), None))

    def step(*args):
        return on_device(*args)

    step = jax.shard_map(
        step, mesh=mesh, in_specs=in_specs, out_specs=out_specs, check_vma=False
    )
    return step
```
